32 devices in a mesh: seq: 8 (over z, y), head: 4 (over x, core).
Axes of the slice: x: 2, y: 2, z: 4, core: 2. Of those that a mesh axis runs over, the one named last changes fastest.
Arguments:
- cache: bfloat16 [1024, 576], P('seq'), may hold values from -8 to 8
- query_nope: bfloat16 [1024, 4096], P('seq', 'head'), may hold values from -5 to 5
- query_rope: bfloat16 [1024, 2048], P('seq', 'head'), may hold values from -256 to 256
- scale_exp: int32 [1024], P('seq'), may hold values from -1 to 1
- offsets: int32 [16], P('seq'), may hold values from 0 to 960
- up_key: bfloat16 [512, 4096], P(None, 'head'), may hold values from -0.25 to 0.25
- up_value: bfloat16 [512, 4096], P(None, 'head'), may hold values from -0.25 to 0.25
- grad_out: bfloat16 [1024, 4096], P('seq', 'head'), may hold values from -5 to 5
Outputs:
- d_cache: bfloat16 [1024, 576], P('seq')
- d_query_nope: bfloat16 [1024, 4096], P('seq', 'head')
- d_query_rope: bfloat16 [1024, 2048], P('seq', 'head')
The draws below stay inside these ranges and needn't reach their ends.
All inputs are finite; a program needn't handle non-finite values.
Results may differ from the reference program's by a relative error of at most 0.0099.
Values may be sent and summed in bfloat16 or wider, within the bound.
A program may use at most 64 MiB of HBM per device.

```python
import jax
import jax.numpy as jnp
from jax import lax

LATENT = 512
ROPE = 64
NOPE = 128
QBLOCK = 64
HEADS = 32
QUERIES = 1024
KEYS = 1024


def shared_draw(key):
    base = jax.random.fold_in(key, 4049)
    exponents = jax.random.randint(jax.random.fold_in(base, 1), (QUERIES,), -1, 2).astype(jnp.int32)
    return exponents


def draw_scale_exp(key, part):
    exponents = shared_draw(key)
    return exponents


def draw_cache(key, part):
    first = jax.random.fold_in(key, 17)
    latent = jnp.clip(jax.random.normal(jax.random.fold_in(first, 4), (KEYS, LATENT), jnp.float32), -4.0, 4.0)
    rotary = jnp.clip(jax.random.normal(jax.random.fold_in(first, 5), (KEYS, ROPE), jnp.float32), -4.0, 4.0)
    return jnp.concatenate([latent, rotary], axis=1).astype(jnp.bfloat16)


def draw_query_rope(key, part):
    first = jax.random.fold_in(key, 29)
    values = jnp.clip(jax.random.normal(jax.random.fold_in(first, 2), (QUERIES, HEADS * ROPE), jnp.float32), -4.0, 4.0)
    return values.astype(jnp.bfloat16)


def set_ends(array, own_key, least, top_value):
    longest = array.shape.index(max(array.shape))
    spots = []
    for shift in (0, 1):
        where = [jax.random.randint(jax.random.fold_in(own_key, axis), (), 0, length) for axis, length in enumerate(array.shape)]
        where[longest] = (where[longest] + shift) % array.shape[longest]
        spots.append(tuple(where))
    return array.at[spots[0]].set(least).at[spots[1]].set(top_value)


def steps_of(rng, dims, cuts, least, top_value):
    factor_of = 1.0
    for position, blocks in cuts:
        heights = jax.random.uniform(jax.random.fold_in(jax.random.fold_in(rng, 6), position), (blocks,), jnp.float32, least / len(cuts), top_value / len(cuts))
        factor_of = factor_of * jnp.repeat(jnp.exp(heights), dims[position] // blocks).reshape((-1,) + (1,) * (len(dims) - 1 - position))
    return factor_of


def normal_values(key, extent, spread, bound, pieces=(), kind=jnp.bfloat16):
    entries = jax.random.normal(key, extent, jnp.float32) * spread
    if len(pieces) > 0:
        entries = steps_of(key, extent, pieces, -0.22, 0.18) * entries
    return jnp.clip(entries, min=-bound, max=bound).astype(kind)


def setup_inputs(seed: int = 0) -> dict:
    splits = jax.random.split(jax.random.key(seed), 9)
    cache = draw_cache(jax.random.fold_in(splits[8], 71), 0)
    query_nope = normal_values(splits[1], (QUERIES, HEADS * NOPE), 1.0, 5.0, ((0, 8), (1, 4)))
    query_rope = draw_query_rope(jax.random.fold_in(splits[8], 71), 0)
    scale_exp = draw_scale_exp(jax.random.fold_in(splits[8], 71), 0)
    offsets = set_ends(jax.random.randint(splits[4], (QUERIES // QBLOCK,), 0, KEYS - QBLOCK + 1), jax.random.fold_in(splits[4], 1), 0, KEYS - QBLOCK).astype(jnp.int32)
    up_key = normal_values(splits[5], (LATENT, HEADS * NOPE), LATENT ** -0.5, 0.25, ((1, 4),))
    up_value = normal_values(splits[6], (LATENT, HEADS * NOPE), LATENT ** -0.5, 0.25, ((1, 4),))
    grad_out = normal_values(splits[7], (QUERIES, HEADS * NOPE), 1.0, 5.0, ((0, 8), (1, 4)))
    return dict(cache=cache, query_nope=query_nope, query_rope=query_rope, scale_exp=scale_exp, offsets=offsets, up_key=up_key, up_value=up_value, grad_out=grad_out)


def reference(cache, query_nope, query_rope, scale_exp, offsets, up_key, up_value, grad_out):
    scale = (NOPE + ROPE) ** -0.5
    factor = jnp.exp2(scale_exp.astype(jnp.float32))[:, None]
    q_nope = (query_nope.astype(jnp.float32) * factor).astype(jnp.bfloat16).reshape(QUERIES, HEADS, NOPE)
    q_rope = (query_rope.astype(jnp.float32) * factor).astype(jnp.bfloat16).reshape(QUERIES, HEADS, ROPE)
    outgrad = grad_out.reshape(QUERIES, HEADS, NOPE)
    w_key = up_key.reshape(LATENT, HEADS, NOPE)
    w_value = up_value.reshape(LATENT, HEADS, NOPE)
    positions = (offsets[:, None] + jnp.arange(QBLOCK, dtype=jnp.int32)[None, :]).reshape(-1)
    visible = jnp.arange(KEYS, dtype=jnp.int32)[None, :] <= positions[:, None]
    latent = cache[:, :LATENT]

    def one_head(total, items):
        head_nope, head_rope, head_key, head_value, head_grad = items
        absorbed = jnp.dot(head_nope, head_key.T, preferred_element_type=jnp.float32).astype(jnp.bfloat16)
        extended = jnp.concatenate([absorbed, head_rope], axis=1)
        back = jnp.dot(head_grad, head_value.T, preferred_element_type=jnp.float32).astype(jnp.bfloat16)
        raw = jnp.dot(extended, cache.T, preferred_element_type=jnp.float32) * scale
        scores = jnp.where(visible, raw, -jnp.inf)
        top = jnp.max(scores, axis=1, keepdims=True)
        lse = top + jnp.log(jnp.sum(jnp.exp(scores - top), axis=1, keepdims=True))
        probs = jnp.exp(scores - lse)
        probs_b = probs.astype(jnp.bfloat16)
        latent_out = jnp.dot(probs_b, latent, preferred_element_type=jnp.float32)
        delta = jnp.sum(back.astype(jnp.float32) * latent_out, axis=1, keepdims=True)
        dprob = jnp.dot(back, latent.T, preferred_element_type=jnp.float32)
        dscore = (probs * (dprob - delta) * scale).astype(jnp.bfloat16)
        grad_ext = jnp.dot(dscore, cache, preferred_element_type=jnp.float32)
        grad_abs = grad_ext[:, :LATENT].astype(jnp.bfloat16)
        dq_nope = jnp.dot(grad_abs, head_key, preferred_element_type=jnp.float32) * factor
        dq_rope = grad_ext[:, LATENT:] * factor
        term = jnp.dot(dscore.T, extended, preferred_element_type=jnp.float32)
        term_value = jnp.dot(probs_b.T, back, preferred_element_type=jnp.float32)
        total = total + term + jnp.pad(term_value, ((0, 0), (0, ROPE)))
        return total, (dq_nope.astype(jnp.bfloat16), dq_rope.astype(jnp.bfloat16))

    items = (jnp.transpose(q_nope, (1, 0, 2)), jnp.transpose(q_rope, (1, 0, 2)),
             jnp.transpose(w_key, (1, 0, 2)), jnp.transpose(w_value, (1, 0, 2)),
             jnp.transpose(outgrad, (1, 0, 2)))
    start = jnp.zeros((KEYS, LATENT + ROPE), jnp.float32)
    total, (dq_nope, dq_rope) = lax.scan(one_head, start, items)
    d_query_nope = jnp.transpose(dq_nope, (1, 0, 2)).reshape(QUERIES, HEADS * NOPE)
    d_query_rope = jnp.transpose(dq_rope, (1, 0, 2)).reshape(QUERIES, HEADS * ROPE)
    return total.astype(jnp.bfloat16), d_query_nope, d_query_rope
```

```python
import functools
import math

import jax
import jax.numpy as jnp
from jax import lax
from jax.experimental import pallas as pl
from jax.experimental.pallas import tpu as pltpu
from jax.sharding import PartitionSpec as P

LATENT = 512
ROPE = 64
NOPE = 128
QBLOCK = 64
MESH = pl.DeviceIdType.MESH
BF16 = jnp.bfloat16
F32 = jnp.float32
NEG = -1e30


def dot(a, b):
    return jnp.dot(a, b, preferred_element_type=F32)


def dot_nt(a, b):
    return lax.dot_general(a, b, (((1,), (1,)), ((), ())), preferred_element_type=F32)


def kernel(
    nz, nx,
    cache_ref, qn_ref, qr_ref, se_ref, off_ref, uk_ref, uv_ref, go_ref,
    dc_ref, dqn_ref, dqr_ref,
    full, cT, extT, ext, backT, back, upkT, S, dP, pT, dsT, mx, D,
    csnd, crcv, ysnd, yrcv, zsnd, zrcv, xsnd, xrcv, fin, rfin,
    gz_send, gy_send, gc_send, g_recv,
    c_send, c_recv, y_send, y_recv, z_send, z_recv, x_send, x_recv, f_send, f_recv,
):
    own, width = cache_ref.shape
    half = own // 2
    pair = 2 * own
    queries = qn_ref.shape[0]
    heads = qn_ref.shape[1] // NOPE
    rows = heads * queries
    scale = (NOPE + ROPE) ** (-0.5)
    s_me = lax.axis_index("seq")
    h_me = lax.axis_index("head")
    z, y = s_me // 2, lax.rem(s_me, 2)
    x, core = h_me // 2, lax.rem(h_me, 2)
    oy, oc = 1 - y, 1 - core

    def z_dev(zz):
        return (zz * 2 + y, h_me)

    y_dev = (z * 2 + oy, h_me)
    c_dev = (s_me, x * 2 + oc)

    def x_dev(xx):
        return (s_me, xx * 2 + core)

    zs = [lax.rem(z + k, nz) for k in range(nz)]
    xs = [lax.rem(x + k, nx) for k in range(nx)]

    barrier = pltpu.get_barrier_semaphore()
    peers = [z_dev(zz) for zz in zs[1:]] + [y_dev, c_dev] + [x_dev(xx) for xx in xs[1:]]
    for dev in peers:
        pl.semaphore_signal(barrier, inc=1, device_id=dev, device_id_type=MESH)
    pl.semaphore_wait(barrier, len(peers))

    def remote(src, dst, send, recv, dev):
        return pltpu.make_async_remote_copy(
            src_ref=src, dst_ref=dst, send_sem=send, recv_sem=recv,
            device_id=dev, device_id_type=MESH,
        )

    def half_rows(blk, hf):
        return pl.ds(pl.multiple_of(blk * own + hf * half, half), half)

    def gather(src, blk, hf, send, dev):
        return remote(src, full.at[half_rows(blk, hf)], send, g_recv.at[blk * 2 + hf], dev)

    sends = []
    mine = cache_ref.at[pl.ds(pl.multiple_of(core * half, half), half)]

    def go(copy):
        copy.start()
        sends.append(copy)

    go(gather(mine, s_me, core, gy_send.at[0], y_dev))
    for k in range(1, nz):
        go(gather(mine, s_me, core, gz_send.at[k], z_dev(zs[k])))

    full[pl.ds(pl.multiple_of(s_me * own, own), own), :] = cache_ref[...]
    factor = jnp.exp2(se_ref[...].astype(F32))
    lane = lax.broadcasted_iota(jnp.int32, (1, queries), 1)
    pos = jnp.zeros((1, queries), jnp.int32)
    for b in range(queries // QBLOCK):
        inside = (lane >= b * QBLOCK) & (lane < (b + 1) * QBLOCK)
        pos = jnp.where(inside, off_ref[b] + lane - b * QBLOCK, pos)

    for h in range(heads):
        cols = slice(h * NOPE, (h + 1) * NOPE)
        qs = slice(h * queries, (h + 1) * queries)
        w = uk_ref[:, cols]
        a = (dot_nt(w, qn_ref[:, cols]) * factor).astype(BF16)
        extT[0:LATENT, qs] = a
        ext[qs, 0:LATENT] = a.T
        upkT[cols, :] = w.T
        g = dot_nt(uv_ref[:, cols], go_ref[:, cols]).astype(BF16)
        backT[:, qs] = g
        back[qs, :] = g.T
    for h in range(0, heads, 2):
        r = (qr_ref[:, h * ROPE : (h + 2) * ROPE].astype(F32).T * factor).astype(BF16)
        for i in range(2):
            part = r[i * ROPE : (i + 1) * ROPE, :]
            qs = slice((h + i) * queries, (h + i + 1) * queries)
            extT[LATENT:width, qs] = part
            ext[qs, LATENT:width] = part.astype(F32).T.astype(BF16)
    mx[...] = jnp.full(mx.shape, NEG, F32)

    tile = 2 * queries
    pos2 = jnp.concatenate([pos, pos], axis=1)

    def scores(zz):
        base = pl.multiple_of(zz * pair, pair)
        c = full[pl.ds(base, pair), :]
        key = base + lax.broadcasted_iota(jnp.int32, (pair, tile), 0)
        seen = key <= pos2
        for t in range(rows // tile):
            ls = slice(t * tile, (t + 1) * tile)
            s = dot(c, extT[:, ls]) * (scale * math.log2(math.e))
            s = jnp.where(seen, s, NEG)
            S[pl.ds(base, pair), ls] = s
            mx[:, ls] = jnp.maximum(mx[:, ls], jnp.max(s.reshape(pair // 8, 8, tile), axis=0))
            dP[pl.ds(base, pair), ls] = dot(c[:, :LATENT], backT[:, ls])
        cT[:, pl.ds(base, pair)] = c.T

    def got(blk, hf):
        gather(mine, blk, hf, gy_send.at[0], c_dev).wait_recv()

    def forward(blk, send, dev):
        go(gather(full.at[half_rows(blk, core)], blk, core, send, dev))

    for k in range(nz + 2):
        if 1 <= k < nz:
            blk = zs[k] * 2 + y
            got(blk, core)
            forward(blk, gy_send.at[k], y_dev)
            forward(blk, gc_send.at[k], c_dev)
        if 1 <= k <= nz:
            blk = zs[k - 1] * 2 + oy
            got(blk, core)
            forward(blk, gc_send.at[nz + k - 1], c_dev)
        if k >= 2:
            zz = zs[k - 2]
            if k > 2:
                got(zz * 2 + y, oc)
            got(zz * 2 + oy, oc)
            scores(zz)

    keys = full.shape[0]
    chunk = own

    def soften(h, carry):
        ls = pl.ds(pl.multiple_of(h * queries, queries), queries)
        top = jnp.max(mx[:, ls], axis=0, keepdims=True)
        tot = jnp.zeros((8, queries), F32)
        dl = jnp.zeros((8, queries), F32)
        for i in range(keys // chunk):
            rs = slice(i * chunk, (i + 1) * chunk)
            p = jnp.exp2(S[rs, ls] - top)
            S[rs, ls] = p
            tot = tot + jnp.sum(p.reshape(chunk // 8, 8, queries), axis=0)
            dl = dl + jnp.sum((p * dP[rs, ls]).reshape(chunk // 8, 8, queries), axis=0)
        inv = 1.0 / jnp.sum(tot, axis=0, keepdims=True)
        delta = jnp.sum(dl, axis=0, keepdims=True) * inv
        for i in range(keys // chunk):
            rs = slice(i * chunk, (i + 1) * chunk)
            pr = S[rs, ls] * inv
            pT[rs, ls] = pr.astype(BF16)
            dsT[rs, ls] = (pr * (dP[rs, ls] - delta) * scale).astype(BF16)
        return carry

    lax.fori_loop(0, heads, soften, 0)

    def core_copy(zz, i):
        return remote(csnd.at[zz], crcv.at[zz], c_send.at[zz], c_recv.at[zz], c_dev)

    def y_copy(zz):
        return remote(ysnd.at[zz], yrcv.at[zz], y_send.at[zz], y_recv.at[zz], y_dev)

    def step_d(k):
        zz = zs[k]
        rs = pl.ds(pl.multiple_of(zz * pair, pair), pair)
        ds, pb = dsT[rs, :], pT[rs, :]
        D[rs, 0:LATENT] = dot(ds, ext[:, 0:LATENT]) + dot(pb, back[...])
        D[rs, LATENT:width] = dot(ds, ext[:, LATENT:width])
        for yy in range(2):
            csnd[zz, yy] = D[half_rows(zz * 2 + yy, oc), :].astype(BF16)
        go(core_copy(zz, 0))

    def step_e(k):
        zz = zs[k]
        core_copy(zz, 0).wait_recv()
        t = D[half_rows(zz * 2 + oy, core), :] + crcv[zz, oy].astype(F32)
        ysnd[zz] = t.astype(BF16)
        go(y_copy(zz))

    def step_f(k):
        zz = zs[k]
        y_copy(zz).wait_recv()
        u = (
            D[half_rows(zz * 2 + y, core), :]
            + crcv[zz, y].astype(F32)
            + yrcv[zz].astype(F32)
        )
        if k:
            zsnd[zz] = u.astype(BF16)
            go(remote(zsnd.at[zz], zrcv.at[z], z_send.at[zz], z_recv.at[z], z_dev(zz)))
        return u

    def grads(h):
        g = dot(cT[...], dsT[:, h * queries : (h + 2) * queries])
        lo = g[0:LATENT].astype(BF16)
        hi = g[LATENT:width]
        ropes = []
        for i in range(2):
            qs = slice(i * queries, (i + 1) * queries)
            cols = slice((h + i) * NOPE, (h + i + 1) * NOPE)
            d = dot(upkT[cols, :], lo[:, qs]) * factor
            dqn_ref[:, cols] = d.T.astype(BF16)
            ropes.append(hi[:, qs] * factor)
        dqr_ref[:, h * ROPE : (h + 2) * ROPE] = jnp.concatenate(ropes, axis=0).T.astype(BF16)

    order = list(range(1, nz)) + [0]
    pieces = list(range(0, heads, 2))
    for i, k in enumerate(order):
        step_d(k)
        if i:
            step_e(order[i - 1])
    grads(pieces.pop(0))
    step_e(order[-1])
    for k in order[:-1]:
        step_f(k)
        if pieces:
            grads(pieces.pop(0))
    while pieces:
        grads(pieces.pop(0))
    v = step_f(0)
    for k in range(1, nz):
        remote(
            zsnd.at[zs[k]], zrcv.at[zs[k]], z_send.at[zs[k]], z_recv.at[zs[k]], z_dev(zs[k])
        ).wait_recv()
        v = v + zrcv[zs[k]].astype(F32)
    vb = v.astype(BF16)
    xsnd[...] = vb
    for k in range(1, nx):
        go(remote(xsnd, xrcv.at[x], x_send.at[xs[k]], x_recv.at[x], x_dev(xs[k])))
    xrcv[x] = vb
    for k in range(1, nx):
        remote(
            xsnd, xrcv.at[xs[k]], x_send.at[xs[k]], x_recv.at[xs[k]], x_dev(xs[k])
        ).wait_recv()
    w = xrcv[0].astype(F32)
    for i in range(1, nx):
        w = w + xrcv[i].astype(F32)
    wb = w.astype(BF16)
    fin[...] = wb
    last = remote(fin, rfin, f_send.at[0], f_recv.at[0], c_dev)
    go(last)
    dc_ref[pl.ds(pl.multiple_of(core * half, half), half), :] = wb
    last.wait_recv()
    dc_ref[pl.ds(pl.multiple_of(oc * half, half), half), :] = rfin[...]
    for copy in sends:
        copy.wait_send()


def solution(mesh):
    seq, head = mesh.shape["seq"], mesh.shape["head"]
    nz, nx = seq // 2, head // 2

    def per_device(cache, qn, qr, se, off, uk, uv, go):
        own, width = cache.shape
        half = own // 2
        keys = own * seq
        queries = qn.shape[0]
        heads = qn.shape[1] // NOPE
        rows = heads * queries
        vm = pltpu.VMEM
        dma = pltpu.SemaphoreType.DMA
        vspec = pl.BlockSpec(memory_space=pltpu.VMEM)
        sspec = pl.BlockSpec(memory_space=pltpu.SMEM)
        return pl.pallas_call(
            functools.partial(kernel, nz, nx),
            out_shape=(
                jax.ShapeDtypeStruct(cache.shape, BF16),
                jax.ShapeDtypeStruct(qn.shape, BF16),
                jax.ShapeDtypeStruct(qr.shape, BF16),
            ),
            in_specs=[vspec, vspec, vspec, vspec, sspec, vspec, vspec, vspec],
            out_specs=(vspec, vspec, vspec),
            scratch_shapes=[
                vm((keys, width), BF16), vm((width, keys), BF16),
                vm((width, rows), BF16), vm((rows, width), BF16),
                vm((LATENT, rows), BF16), vm((rows, LATENT), BF16),
                vm((heads * NOPE, LATENT), BF16),
                vm((keys, rows), F32), vm((keys, rows), F32),
                vm((keys, rows), BF16), vm((keys, rows), BF16),
                vm((8, rows), F32), vm((keys, width), F32),
                vm((nz, 2, half, width), BF16), vm((nz, 2, half, width), BF16),
                vm((nz, half, width), BF16), vm((nz, half, width), BF16),
                vm((nz, half, width), BF16), vm((nz, half, width), BF16),
                vm((half, width), BF16), vm((nx, half, width), BF16),
                vm((half, width), BF16), vm((half, width), BF16),
                dma((nz,)), dma((nz,)), dma((2 * nz,)), dma((2 * seq,)),
                dma((nz,)), dma((nz,)), dma((nz,)), dma((nz,)),
                dma((nz,)), dma((nz,)), dma((nx,)), dma((nx,)), dma((1,)), dma((1,)),
            ],
            compiler_params=pltpu.CompilerParams(
                collective_id=0, has_side_effects=True, vmem_limit_bytes=60 * 1024 * 1024
            ),
        )(cache, qn, qr, se.reshape(1, -1), off, uk, uv, go)

    in_specs = (
        P("seq", None), P("seq", "head"), P("seq", "head"), P("seq"), P("seq"),
        P(None, "head"), P(None, "head"), P("seq", "head"),
    )
    out_specs = (P("seq", None), P("seq", "head"), P("seq", "head"))
    return jax.shard_map(
        per_device, mesh=mesh, in_specs=in_specs, out_specs=out_specs, check_vma=False
    )
```
